32 devices in a mesh: dom: 16 (over z, y, x), tp: 2 (over core).
Axes of the slice: x: 2, y: 2, z: 4, core: 2. Of those that a mesh axis runs over, the one named last changes fastest.
Arguments:
- node_latent: bfloat16 [16384, 128], P('dom'), may hold values from -6 to 6
- edge_latent: bfloat16 [131072, 128], P(('dom', 'tp')), may hold values from -6 to 6
- edge_sender: int32 [131072], P(('dom', 'tp')), may hold values from 0 to 1535, as said below
- edge_receiver: int32 [131072], P(('dom', 'tp')), may hold values from 0 to 1535, as said below
- edge_count: int32 [32], P(('dom', 'tp')), may hold values from 2048 to 4096, as said below
- send_index: int32 [16, 4, 128], P('dom'), may hold values from -1 to 1023, as said below
- edge_in: bfloat16 [3, 384, 128], P(None, None, 'tp'), may hold values from -0.3125 to 0.3125
- edge_out: bfloat16 [3, 128, 128], P(None, 'tp'), may hold values from -0.5 to 0.5
- node_in: bfloat16 [3, 256, 128], P(None, None, 'tp'), may hold values from -0.375 to 0.375
- node_out: bfloat16 [3, 128, 128], P(None, 'tp'), may hold values from -0.5 to 0.5
Outputs:
- node_result: bfloat16 [16384, 128], P('dom')
- edge_result: bfloat16 [131072, 128], P(('dom', 'tp'))
The draws below stay inside these ranges and needn't reach their ends.
Inputs may be any that keep to these rules, and one draw needn't show every extreme that they name: `send_index`: entry [p, k, j] is a local node index of partition p sent to partition (p + o_k) mod 16, with o = (1, -1, 2, -2); -1 marks padding, which stands only after the live entries of a block; live entries of a block are distinct; at least half of each block is live and some block is full. `edge_sender`: an index below 1024 is an owned node of the slot's partition; index 1024 + k * 128 + j is slot j of halo block k; never a padding halo slot. `edge_receiver`: as for edge_sender. `edge_count`: some device block is full.
All inputs are finite; a program needn't handle non-finite values.
Results may differ from the reference program's by a relative error of at most 0.013.
Values may be sent and summed in bfloat16 or wider, within the bound.
No kernel may reach another device: no remote copies, remote signals or barrier semaphores. Data moves between devices by JAX's collectives and lax.ppermute only.
A program may use at most 64 MiB of HBM per device.

```python
import jax
import jax.numpy as jnp
from jax import lax

L = 128
H = 128
NODE_DEV = 1024
SLOT = 128
PEERS = 4
LAYERS = 3
EDGE_DEV = 4096
DOMAINS = 16
SHARDS = 32
NODES = 16384
EDGES = 131072


neighbour_offsets = (1, -1, 2, -2)


def halo_counts(key):
    counts = jax.random.randint(jax.random.fold_in(key, 11), (DOMAINS, PEERS), SLOT // 2, SLOT + 1)
    chosen = jax.random.randint(jax.random.fold_in(key, 12), (2,), 0, 1 << 20)
    counts = counts.at[chosen[0] % DOMAINS, chosen[1] % PEERS].set(SLOT)
    return counts.astype(jnp.int32)


def incoming_counts(key):
    counts = halo_counts(key)
    columns = [jnp.roll(counts[:, neighbour], offset) for neighbour, offset in enumerate(neighbour_offsets)]
    return jnp.stack(columns, axis=1)


def draw_send_index(key, part):
    counts = halo_counts(key)
    subkeys = jax.random.split(jax.random.fold_in(key, 13), DOMAINS * PEERS)
    chosen = jax.vmap(lambda subkey: jax.random.permutation(subkey, NODE_DEV)[:SLOT])(subkeys)
    chosen = chosen.reshape(DOMAINS, PEERS, SLOT)
    position = jnp.arange(SLOT, dtype=jnp.int32)[None, None, :]
    return jnp.where(position < counts[:, :, None], chosen, -1).astype(jnp.int32)


def endpoints(key, salt, halo_share):
    inbound = incoming_counts(key)
    base = jax.random.fold_in(key, salt)
    first_key, second_key, third_key, fourth_key = jax.random.split(base, 4)
    shape = (SHARDS, EDGE_DEV)
    owned_pick = jax.random.randint(first_key, shape, 0, NODE_DEV)
    block_pick = jax.random.randint(second_key, shape, 0, PEERS)
    raw_bits = jax.random.randint(third_key, shape, 0, 1 << 20)
    domain_of = (jnp.arange(SHARDS, dtype=jnp.int32) // (SHARDS // DOMAINS))[:, None]
    limit = inbound[domain_of, block_pick]
    halo_pick = NODE_DEV + block_pick * SLOT + raw_bits % limit
    use_halo = jax.random.randint(fourth_key, shape, 0, 100) < halo_share
    return jnp.where(use_halo, halo_pick, owned_pick).astype(jnp.int32).reshape(EDGES)


def draw_edge_sender(key, part):
    return endpoints(key, 21, 20)


def draw_edge_receiver(key, part):
    return endpoints(key, 22, 10)


def draw_edge_count(key, part):
    counts = jax.random.randint(jax.random.fold_in(key, 31), (SHARDS,), EDGE_DEV // 2, EDGE_DEV + 1)
    filled = jax.random.randint(jax.random.fold_in(key, 32), (), 0, SHARDS)
    return counts.at[filled].set(EDGE_DEV).astype(jnp.int32)


def block_levels(rng, dims, cuts, least, largest):
    level, own = 1.0, jax.random.fold_in(rng, 6)
    for axis_at, shards_of in cuts:
        heights = jnp.exp(jax.random.uniform(jax.random.fold_in(own, axis_at), (shards_of,), jnp.float32, least / len(cuts), largest / len(cuts)))
        level = level * jnp.repeat(heights, dims[axis_at] // shards_of).reshape([-1 if axis == axis_at else 1 for axis in range(len(dims))])
    return level


def bell_draw(rng, dims, width, bound, cuts=(), held_as=jnp.bfloat16):
    entries = jax.random.normal(rng, dims, jnp.float32) * width
    if len(cuts) > 0:
        entries = block_levels(rng, dims, cuts, -0.22, 0.18) * entries
    return jnp.clip(entries, min=-bound, max=bound).astype(held_as)


def setup_inputs(seed: int = 0) -> dict:
    arg_keys = jax.random.split(jax.random.key(seed), 11)
    node_latent = bell_draw(arg_keys[0], (NODES, L), 1.0, 6.0, ((0, 16),))
    edge_latent = bell_draw(arg_keys[1], (EDGES, L), 1.0, 6.0, ((0, 32),))
    edge_sender = draw_edge_sender(jax.random.fold_in(arg_keys[10], 71), 0)
    edge_receiver = draw_edge_receiver(jax.random.fold_in(arg_keys[10], 71), 0)
    edge_count = draw_edge_count(jax.random.fold_in(arg_keys[10], 71), 0)
    send_index = draw_send_index(jax.random.fold_in(arg_keys[10], 71), 0)
    edge_in = bell_draw(arg_keys[6], (LAYERS, 3 * L, H), (3 * L) ** -0.5, 0.3125, ((2, 2),))
    edge_out = bell_draw(arg_keys[7], (LAYERS, H, L), H ** -0.5, 0.5, ((1, 2),))
    node_in = bell_draw(arg_keys[8], (LAYERS, 2 * L, H), (2 * L) ** -0.5, 0.375, ((2, 2),))
    node_out = bell_draw(arg_keys[9], (LAYERS, H, L), H ** -0.5, 0.5, ((1, 2),))
    return {"node_latent": node_latent, "edge_latent": edge_latent, "edge_sender": edge_sender, "edge_receiver": edge_receiver, "edge_count": edge_count, "send_index": send_index, "edge_in": edge_in, "edge_out": edge_out, "node_in": node_in, "node_out": node_out}


neighbour_offsets = (1, -1, 2, -2)
norm_floor = 0.25

def layer_norm(values):
    centre = lax.optimization_barrier(jnp.mean(values, axis=-1, keepdims=True))
    centred = values - centre
    spread = lax.optimization_barrier(jnp.mean(centred * centred, axis=-1, keepdims=True))
    return centred * lax.rsqrt(spread + norm_floor)

def product(first_operand, second_operand):
    return jnp.dot(first_operand, second_operand, preferred_element_type=jnp.float32)

def reference(node_latent, edge_latent, edge_sender, edge_receiver, edge_count, send_index, edge_in, edge_out, node_in, node_out):
    feature_width = node_latent.shape[1]
    shard_count = SHARDS // DOMAINS
    extended_rows = NODE_DEV + PEERS * SLOT
    nodes_now = node_latent.reshape(DOMAINS, NODE_DEV, feature_width)
    edges_now = edge_latent.reshape(DOMAINS, shard_count * EDGE_DEV, feature_width)
    senders = edge_sender.reshape(DOMAINS, shard_count * EDGE_DEV)
    receivers = edge_receiver.reshape(DOMAINS, shard_count * EDGE_DEV)
    live_edges = (jnp.arange(EDGE_DEV, dtype=jnp.int32)[None, :] < edge_count[:, None]).reshape(DOMAINS, shard_count * EDGE_DEV)
    usable = send_index >= 0
    safe_index = jnp.where(usable, send_index, 0).astype(jnp.int32)
    domain_ids = jnp.arange(DOMAINS, dtype=jnp.int32)[:, None]
    for layer_index in range(LAYERS):
        picked = nodes_now[domain_ids[:, :, None], safe_index]
        picked = jnp.where(usable[..., None], picked, jnp.zeros((), jnp.bfloat16))
        halo_rows = jnp.stack([jnp.roll(picked[:, neighbour], offset, axis=0) for neighbour, offset in enumerate(neighbour_offsets)], axis=1)
        extended = jnp.concatenate([nodes_now, halo_rows.reshape(DOMAINS, PEERS * SLOT, feature_width)], axis=1)
        weight_in = edge_in[layer_index]
        weight_out = edge_out[layer_index]

        def edge_step(operands):
            extended_part, latent, sender_ids, receiver_ids, live_mask = operands
            linear = product(latent, weight_in[:feature_width])
            linear = linear + product(extended_part[sender_ids], weight_in[feature_width:2 * feature_width])
            linear = linear + product(extended_part[receiver_ids], weight_in[2 * feature_width:])
            edge_hidden = jnp.maximum(linear, 0.0).astype(jnp.bfloat16)
            message = jnp.where(live_mask[:, None], layer_norm(product(edge_hidden, weight_out)), 0.0).astype(jnp.bfloat16)
            message = lax.optimization_barrier(message)
            wide_message = message.astype(jnp.float32)
            renewed = (latent.astype(jnp.float32) + wide_message).astype(jnp.bfloat16)
            summed_part = jax.ops.segment_sum(wide_message, receiver_ids, num_segments=extended_rows)
            return (renewed, summed_part)
        edges_now, summed = lax.map(edge_step, (extended, edges_now, senders, receivers, live_edges))
        owned_sums = summed[:, :NODE_DEV]
        returned = summed[:, NODE_DEV:].reshape(DOMAINS, PEERS, SLOT, feature_width)
        for neighbour, offset in enumerate(neighbour_offsets):
            arrived = jnp.roll(returned[:, neighbour], -offset, axis=0)
            arrived = jnp.where(usable[:, neighbour, :, None], arrived, 0.0)
            owned_sums = owned_sums.at[domain_ids, safe_index[:, neighbour]].add(arrived)
        aggregate = owned_sums.astype(jnp.bfloat16).reshape(DOMAINS * NODE_DEV, feature_width)
        flat_nodes = nodes_now.reshape(DOMAINS * NODE_DEV, feature_width)
        first_weight = node_in[layer_index]
        linear_nodes = product(flat_nodes, first_weight[:feature_width]) + product(aggregate, first_weight[feature_width:])
        node_hidden = jnp.maximum(linear_nodes, 0.0).astype(jnp.bfloat16)
        update = layer_norm(product(node_hidden, node_out[layer_index]))
        nodes_now = (flat_nodes.astype(jnp.float32) + update).astype(jnp.bfloat16).reshape(DOMAINS, NODE_DEV, feature_width)
    return (nodes_now.reshape(NODES, feature_width), edges_now.reshape(EDGES, feature_width))
```

```python
import functools

import jax
import jax.numpy as jnp
from jax import lax
from jax.experimental import pallas as pl
from jax.experimental.pallas import tpu as pltpu
from jax.sharding import PartitionSpec as P

LAYERS = 3

neighbour_offsets = (1, -1, 2, -2)
norm_floor = 0.25
LANES = 128


def from_behind(array, axis, by):
    length = lax.axis_size(axis)
    return lax.ppermute(array, axis, [(i, (i + by) % length) for i in range(length)])


def layer_norm(values):
    centre = jnp.mean(values, axis=-1, keepdims=True)
    centred = values - centre
    spread = jnp.mean(centred * centred, axis=-1, keepdims=True)
    return centred * lax.rsqrt(spread + norm_floor)


def product(first_operand, second_operand):
    return jnp.dot(first_operand, second_operand, preferred_element_type=jnp.float32)


def one_hot_rows(wide_ids, columns):
    lane = lax.broadcasted_iota(jnp.int16, wide_ids.shape, 1)
    one = jnp.ones((), jnp.bfloat16)
    zero = jnp.zeros((), jnp.bfloat16)
    return [
        jnp.where(wide_ids == lane + jnp.int16(start), one, zero)
        for start in range(0, columns, LANES)
    ]


def edge_kernel(
    count, sender, receiver, receiver_row, latent, nodes, halo, w_in, w_out,
    renewed, owned, returned, table, sums,
):
    step = pl.program_id(0)
    feature_width = latent.shape[1]
    block_rows = latent.shape[0]
    node_total = nodes.shape[0]
    extended_total = node_total + halo.shape[0]

    @pl.when(step == 0)
    def _():
        w = w_in[...]
        table[:feature_width] = w[:feature_width]
        for part in range(2):
            base = feature_width + part * extended_total
            weight = w[(part + 1) * feature_width : (part + 2) * feature_width]
            table[base : base + node_total] = product(nodes[...], weight).astype(jnp.bfloat16)
            table[base + node_total : base + extended_total] = product(halo[...], weight).astype(
                jnp.bfloat16
            )
        sums[...] = jnp.zeros_like(sums)

    edges = latent[...]
    selector = jnp.concatenate(
        [edges]
        + one_hot_rows(sender[...], extended_total)
        + one_hot_rows(receiver[...], extended_total),
        axis=1,
    )
    hidden = jnp.maximum(product(selector, table[...]), 0.0).astype(jnp.bfloat16)
    row = step * block_rows + lax.broadcasted_iota(jnp.int32, (block_rows, feature_width), 0)
    message = jnp.where(row < count[0], layer_norm(product(hidden, w_out[...])), 0.0).astype(
        jnp.bfloat16
    )
    renewed[...] = (edges.astype(jnp.float32) + message.astype(jnp.float32)).astype(jnp.bfloat16)
    ids = jnp.broadcast_to(receiver_row[0], (extended_total, block_rows))
    node = lax.broadcasted_iota(jnp.int32, (extended_total, block_rows), 0)
    spread = jnp.where(ids == node, 1.0, 0.0).astype(jnp.bfloat16)
    sums[...] += product(spread, message)

    @pl.when(step == pl.num_programs(0) - 1)
    def _():
        owned[...] = sums[:node_total]
        returned[...] = sums[node_total:].astype(jnp.bfloat16)


def edge_step(count, sender, receiver, receiver_row, latent, nodes, halo, w_in, w_out):
    edge_rows, feature_width = latent.shape
    block_rows = receiver_row.shape[2]
    node_total = nodes.shape[0]
    halo_total = halo.shape[0]
    extended_total = node_total + halo_total
    whole = lambda array: pl.BlockSpec(array.shape, lambda i: (0, 0))
    per_block = lambda width: pl.BlockSpec((block_rows, width), lambda i: (i, 0))
    return pl.pallas_call(
        edge_kernel,
        grid=(edge_rows // block_rows,),
        in_specs=[
            pl.BlockSpec(memory_space=pltpu.SMEM),
            per_block(LANES),
            per_block(LANES),
            pl.BlockSpec((1, 1, block_rows), lambda i: (i, 0, 0)),
            per_block(feature_width),
            whole(nodes),
            whole(halo),
            whole(w_in),
            whole(w_out),
        ],
        out_specs=[
            per_block(feature_width),
            pl.BlockSpec((node_total, feature_width), lambda i: (0, 0)),
            pl.BlockSpec((halo_total, feature_width), lambda i: (0, 0)),
        ],
        out_shape=[
            jax.ShapeDtypeStruct(latent.shape, jnp.bfloat16),
            jax.ShapeDtypeStruct((node_total, feature_width), jnp.float32),
            jax.ShapeDtypeStruct((halo_total, feature_width), jnp.bfloat16),
        ],
        scratch_shapes=[
            pltpu.VMEM((feature_width + 2 * extended_total, feature_width), jnp.bfloat16),
            pltpu.VMEM((extended_total, feature_width), jnp.float32),
        ],
        name="edge_step",
    )(count, sender, receiver, receiver_row, latent, nodes, halo, w_in, w_out)


def exchange(blocks, directions):
    return [
        from_behind(block, "dom", sign * offset)
        for block, offset, sign in zip(blocks, neighbour_offsets, directions)
    ]


def local(
    node_latent,
    edge_latent,
    edge_sender,
    edge_receiver,
    edge_count,
    send_index,
    edge_in,
    edge_out,
    node_in,
    node_out,
):
    feature_width = node_latent.shape[1]
    node_total = node_latent.shape[0]
    edge_rows = edge_latent.shape[0]
    block_rows = min(512, edge_rows)
    peers, slot = send_index.shape[1:]
    flat_index = send_index[0].reshape(-1)
    node_ids = jnp.arange(node_total, dtype=jnp.int32)
    pick_table = (flat_index[:, None] == node_ids[None, :]).astype(jnp.bfloat16)
    spread_table = (node_ids[:, None] == flat_index[None, :]).astype(jnp.bfloat16)
    wide = lambda ids: jnp.broadcast_to(ids.astype(jnp.int16)[:, None], (edge_rows, LANES))
    sender = wide(edge_sender)
    receiver = wide(edge_receiver)
    receiver_row = edge_receiver.reshape(edge_rows // block_rows, 1, block_rows)
    full_in, full_out = (
        lax.all_gather(edge_in, "tp", axis=2, tiled=True),
        lax.all_gather(edge_out, "tp", axis=1, tiled=True),
    )
    node_first, node_second = (
        lax.all_gather(node_in, "tp", axis=2, tiled=True),
        lax.all_gather(node_out, "tp", axis=1, tiled=True),
    )
    nodes_now = node_latent
    edges_now = edge_latent
    ones = (1,) * peers
    for layer in range(LAYERS):
        picked = product(pick_table, nodes_now).astype(jnp.bfloat16)
        picked = picked.reshape(peers, slot, feature_width)
        halo = jnp.concatenate(exchange([picked[k] for k in range(peers)], ones), axis=0)
        edges_now, owned, returned = edge_step(
            edge_count, sender, receiver, receiver_row, edges_now, nodes_now, halo,
            full_in[layer], full_out[layer],
        )
        returned = returned.reshape(peers, slot, feature_width)
        arrived = exchange([returned[k] for k in range(peers)], (-1,) * peers)
        mine = owned + product(spread_table, jnp.concatenate(arrived, axis=0))
        mine = mine.astype(jnp.bfloat16)
        other = from_behind(mine, "tp", 1)
        aggregate = (mine.astype(jnp.float32) + other.astype(jnp.float32)).astype(jnp.bfloat16)
        linear = product(nodes_now, node_first[layer][:feature_width]) + product(
            aggregate, node_first[layer][feature_width:]
        )
        hidden = jnp.maximum(linear, 0.0).astype(jnp.bfloat16)
        update = layer_norm(product(hidden, node_second[layer]))
        nodes_now = (nodes_now.astype(jnp.float32) + update).astype(jnp.bfloat16)
    return (nodes_now, edges_now)


def solution(mesh):
    return jax.shard_map(
        local,
        mesh=mesh,
        in_specs=(
            P("dom", None),
            P(("dom", "tp"), None),
            P(("dom", "tp")),
            P(("dom", "tp")),
            P(("dom", "tp")),
            P("dom", None, None),
            P(None, None, "tp"),
            P(None, "tp", None),
            P(None, None, "tp"),
            P(None, "tp", None),
        ),
        out_specs=(P("dom", None), P(("dom", "tp"), None)),
        check_vma=False,
    )
```

```python
import functools

import jax
import jax.numpy as jnp
from jax import lax
from jax.experimental import pallas as pl
from jax.experimental.pallas import tpu as pltpu
from jax.sharding import PartitionSpec as P

LAYERS = 3

neighbour_offsets = (1, -1, 2, -2)
norm_floor = 0.25
LANES = 128
EIGHT = jnp.float8_e4m3fn
TABLE_TOP = 384.0
MESSAGE_SCALE = 32.0


def from_behind(array, axis, by):
    length = lax.axis_size(axis)
    return lax.ppermute(array, axis, [(i, (i + by) % length) for i in range(length)])


def layer_norm(values):
    centre = jnp.mean(values, axis=-1, keepdims=True)
    centred = values - centre
    spread = jnp.mean(centred * centred, axis=-1, keepdims=True)
    return centred * lax.rsqrt(spread + norm_floor)


def product(first_operand, second_operand):
    return jnp.dot(first_operand, second_operand, preferred_element_type=jnp.float32)


def one_hot_rows(wide_ids, columns):
    lane = lax.broadcasted_iota(jnp.int16, wide_ids.shape, 1)
    one = jnp.ones((), jnp.bfloat16)
    zero = jnp.zeros((), jnp.bfloat16)
    return [
        jnp.where(wide_ids == lane + jnp.int16(start), one, zero).astype(EIGHT)
        for start in range(0, columns, LANES)
    ]


def split(values):
    high = values.astype(EIGHT)
    low = (values - high.astype(jnp.float32)).astype(EIGHT)
    return jnp.concatenate([high, low], axis=1)


def joined(values):
    half = values.shape[1] // 2
    return values[:, :half] + values[:, half:]


def edge_kernel(
    count, sender, receiver, receiver_row, latent, nodes, halo, w_in, w_out,
    renewed, owned, returned, raw, table, scale, sums,
):
    step = pl.program_id(0)
    feature_width = latent.shape[1]
    block_rows = latent.shape[0]
    node_total = nodes.shape[0]
    extended_total = node_total + halo.shape[0]

    @pl.when(step == 0)
    def _():
        w = w_in[...]
        for part in range(2):
            base = part * extended_total
            weight = w[(part + 1) * feature_width : (part + 2) * feature_width]
            raw[base : base + node_total] = product(nodes[...], weight)
            raw[base + node_total : base + extended_total] = product(halo[...], weight)
        top = jnp.maximum(jnp.max(jnp.abs(raw[...])), 1e-20)
        scale[0] = top / TABLE_TOP
        table[...] = split(raw[...] * (TABLE_TOP / top))
        sums[...] = jnp.zeros_like(sums)

    edges = latent[...]
    selector = jnp.concatenate(
        one_hot_rows(sender[...], extended_total) + one_hot_rows(receiver[...], extended_total),
        axis=1,
    )
    linear = product(edges, w_in[:feature_width])
    linear = linear + joined(product(selector, table[...])) * scale[0]
    hidden = jnp.maximum(linear, 0.0).astype(jnp.bfloat16)
    row = step * block_rows + lax.broadcasted_iota(jnp.int32, (block_rows, feature_width), 0)
    message = jnp.where(row < count[0], layer_norm(product(hidden, w_out[...])), 0.0).astype(
        jnp.bfloat16
    )
    renewed[...] = (edges.astype(jnp.float32) + message.astype(jnp.float32)).astype(jnp.bfloat16)
    ids = jnp.broadcast_to(receiver_row[0].astype(jnp.int16), (LANES, block_rows))
    node = lax.broadcasted_iota(jnp.int16, (LANES, block_rows), 0)
    parts = split(message.astype(jnp.float32) * MESSAGE_SCALE)
    one = jnp.ones((), jnp.bfloat16)
    zero = jnp.zeros((), jnp.bfloat16)
    spread = jnp.concatenate(
        [
            jnp.where(ids == node + jnp.int16(start), one, zero).astype(EIGHT)
            for start in range(0, extended_total, LANES)
        ],
        axis=0,
    )
    sums[...] += joined(product(spread, parts))

    @pl.when(step == pl.num_programs(0) - 1)
    def _():
        owned[...] = sums[:node_total] * (1.0 / MESSAGE_SCALE)
        returned[...] = (sums[node_total:] * (1.0 / MESSAGE_SCALE)).astype(jnp.bfloat16)


def edge_step(count, sender, receiver, receiver_row, latent, nodes, halo, w_in, w_out):
    edge_rows, feature_width = latent.shape
    block_rows = receiver_row.shape[2]
    node_total = nodes.shape[0]
    halo_total = halo.shape[0]
    extended_total = node_total + halo_total
    whole = lambda array: pl.BlockSpec(array.shape, lambda i: (0, 0))
    per_block = lambda width: pl.BlockSpec((block_rows, width), lambda i: (i, 0))
    return pl.pallas_call(
        edge_kernel,
        grid=(edge_rows // block_rows,),
        in_specs=[
            pl.BlockSpec(memory_space=pltpu.SMEM),
            per_block(LANES),
            per_block(LANES),
            pl.BlockSpec((1, 1, block_rows), lambda i: (i, 0, 0)),
            per_block(feature_width),
            whole(nodes),
            whole(halo),
            whole(w_in),
            whole(w_out),
        ],
        out_specs=[
            per_block(feature_width),
            pl.BlockSpec((node_total, feature_width), lambda i: (0, 0)),
            pl.BlockSpec((halo_total, feature_width), lambda i: (0, 0)),
        ],
        out_shape=[
            jax.ShapeDtypeStruct(latent.shape, jnp.bfloat16),
            jax.ShapeDtypeStruct((node_total, feature_width), jnp.float32),
            jax.ShapeDtypeStruct((halo_total, feature_width), jnp.bfloat16),
        ],
        scratch_shapes=[
            pltpu.VMEM((2 * extended_total, feature_width), jnp.float32),
            pltpu.VMEM((2 * extended_total, 2 * feature_width), EIGHT),
            pltpu.SMEM((1,), jnp.float32),
            pltpu.VMEM((extended_total, feature_width), jnp.float32),
        ],
        name="edge_step",
    )(count, sender, receiver, receiver_row, latent, nodes, halo, w_in, w_out)


def across(block, step_of_core):
    domains = lax.axis_size("dom")
    cores = lax.axis_size("tp")
    pairs = [
        (p * cores + t, ((p + step_of_core[t]) % domains) * cores + t)
        for p in range(domains)
        for t in range(cores)
    ]
    return lax.ppermute(block, ("dom", "tp"), pairs)


def swap(array):
    return from_behind(array, "tp", 1)


def in_core_order(mine, other, axis):
    first = lax.axis_index("tp") == 0
    return jnp.concatenate(
        [jnp.where(first, mine, other), jnp.where(first, other, mine)], axis=axis
    )


def local(
    node_latent,
    edge_latent,
    edge_sender,
    edge_receiver,
    edge_count,
    send_index,
    edge_in,
    edge_out,
    node_in,
    node_out,
):
    feature_width = node_latent.shape[1]
    node_total = node_latent.shape[0]
    edge_rows = edge_latent.shape[0]
    block_rows = min(512, edge_rows)
    peers, slot = send_index.shape[1:]
    flat_index = send_index[0].reshape(-1)
    node_ids = jnp.arange(node_total, dtype=jnp.int32)
    cores = lax.axis_size("tp")
    per_core = peers // cores
    own_rows = per_core * slot
    own_steps = [
        tuple(neighbour_offsets[t * per_core + j] for t in range(cores)) for j in range(per_core)
    ]
    core = lax.axis_index("tp")
    own_index = lax.dynamic_slice_in_dim(flat_index, core * own_rows, own_rows)
    pick_table = (own_index[:, None] == node_ids[None, :]).astype(jnp.bfloat16)
    spread_table = (node_ids[:, None] == own_index[None, :]).astype(jnp.bfloat16)

    def placed(ids):
        slot_at = (ids - node_total + (cores - core) * own_rows) % (peers * slot)
        return jnp.where(ids < node_total, ids, node_total + slot_at)

    edge_sender = placed(edge_sender)
    edge_receiver = placed(edge_receiver)
    wide = lambda ids: jnp.broadcast_to(ids.astype(jnp.int16)[:, None], (edge_rows, LANES))
    sender = wide(edge_sender)
    receiver = wide(edge_receiver)
    receiver_row = edge_receiver.reshape(edge_rows // block_rows, 1, block_rows)
    full_in = jnp.concatenate([edge_in, swap(edge_in)], axis=2)
    full_out = jnp.concatenate([edge_out, swap(edge_out)], axis=1)
    node_first = in_core_order(node_in, swap(node_in), 2)
    node_second = in_core_order(node_out, swap(node_out), 1)
    nodes_now = node_latent
    edges_now = edge_latent
    for layer in range(LAYERS):
        picked = product(pick_table, nodes_now).astype(jnp.bfloat16)
        fetched = [
            across(picked[j * slot : (j + 1) * slot], own_steps[j]) for j in range(per_core)
        ]
        fetched = jnp.concatenate(fetched, axis=0)
        halo = jnp.concatenate([fetched, swap(fetched)], axis=0)
        edges_now, owned, returned = edge_step(
            edge_count, sender, receiver, receiver_row, edges_now, nodes_now, halo,
            full_in[layer], full_out[layer],
        )
        sums = returned[:own_rows].astype(jnp.float32) + swap(returned[own_rows:]).astype(
            jnp.float32
        )
        sums = sums.astype(jnp.bfloat16)
        arrived = [
            across(sums[j * slot : (j + 1) * slot], [-o for o in own_steps[j]])
            for j in range(per_core)
        ]
        mine = owned + product(spread_table, jnp.concatenate(arrived, axis=0))
        mine = mine.astype(jnp.bfloat16)
        other = swap(mine)
        aggregate = (mine.astype(jnp.float32) + other.astype(jnp.float32)).astype(jnp.bfloat16)
        linear = product(nodes_now, node_first[layer][:feature_width]) + product(
            aggregate, node_first[layer][feature_width:]
        )
        hidden = jnp.maximum(linear, 0.0).astype(jnp.bfloat16)
        update = layer_norm(product(hidden, node_second[layer]))
        nodes_now = (nodes_now.astype(jnp.float32) + update).astype(jnp.bfloat16)
    return (nodes_now, edges_now)


def solution(mesh):
    return jax.shard_map(
        local,
        mesh=mesh,
        in_specs=(
            P("dom", None),
            P(("dom", "tp"), None),
            P(("dom", "tp")),
            P(("dom", "tp")),
            P(("dom", "tp")),
            P("dom", None, None),
            P(None, None, "tp"),
            P(None, "tp", None),
            P(None, None, "tp"),
            P(None, "tp", None),
        ),
        out_specs=(P("dom", None), P(("dom", "tp"), None)),
        check_vma=False,
    )
```

```python
import functools

import jax
import jax.numpy as jnp
from jax import lax
from jax.experimental import pallas as pl
from jax.experimental.pallas import tpu as pltpu
from jax.sharding import PartitionSpec as P

LAYERS = 3

neighbour_offsets = (1, -1, 2, -2)
norm_floor = 0.25
LANES = 128
EIGHT = jnp.float8_e4m3fn
TABLE_TOP = 384.0
MESSAGE_SCALE = 32.0


def from_behind(array, axis, by):
    length = lax.axis_size(axis)
    return lax.ppermute(array, axis, [(i, (i + by) % length) for i in range(length)])


def layer_norm(values):
    centre = jnp.mean(values, axis=-1, keepdims=True)
    centred = values - centre
    spread = jnp.mean(centred * centred, axis=-1, keepdims=True)
    return centred * lax.rsqrt(spread + norm_floor)


def product(first_operand, second_operand):
    return jnp.dot(first_operand, second_operand, preferred_element_type=jnp.float32)


def one_hot_rows(wide_ids, columns):
    lane = lax.broadcasted_iota(jnp.int16, wide_ids.shape, 1)
    one = jnp.ones((), jnp.bfloat16)
    zero = jnp.zeros((), jnp.bfloat16)
    return [
        jnp.where(wide_ids == lane + jnp.int16(start), one, zero).astype(EIGHT)
        for start in range(0, columns, LANES)
    ]


def split(values):
    high = values.astype(EIGHT)
    low = (values - high.astype(jnp.float32)).astype(EIGHT)
    return jnp.concatenate([high, low], axis=1)


def joined(values):
    half = values.shape[1] // 2
    return values[:, :half] + values[:, half:]


def edge_kernel(
    count, sender, receiver, receiver_row, latent, nodes, halo, w_in, w_out,
    renewed, owned, returned, raw, table, scale, sums,
):
    step = pl.program_id(0)
    feature_width = latent.shape[1]
    block_rows = latent.shape[0]
    node_total = nodes.shape[0]
    extended_total = node_total + halo.shape[0]

    @pl.when(step == 0)
    def _():
        w = w_in[...]
        for part in range(2):
            base = part * extended_total
            weight = w[(part + 1) * feature_width : (part + 2) * feature_width]
            raw[base : base + node_total] = product(nodes[...], weight)
            raw[base + node_total : base + extended_total] = product(halo[...], weight)
        top = jnp.maximum(jnp.max(jnp.abs(raw[...])), 1e-20)
        scale[0] = top / TABLE_TOP
        table[...] = split(raw[...] * (TABLE_TOP / top))
        sums[...] = jnp.zeros_like(sums)

    edges = latent[...]
    selector = jnp.concatenate(
        one_hot_rows(sender[...], extended_total) + one_hot_rows(receiver[...], extended_total),
        axis=1,
    )
    linear = product(edges, w_in[:feature_width])
    linear = linear + joined(product(selector, table[...])) * scale[0]
    hidden = jnp.maximum(linear, 0.0).astype(jnp.bfloat16)
    row = step * block_rows + lax.broadcasted_iota(jnp.int32, (block_rows, feature_width), 0)
    message = jnp.where(row < count[0], layer_norm(product(hidden, w_out[...])), 0.0).astype(
        jnp.bfloat16
    )
    renewed[...] = (edges.astype(jnp.float32) + message.astype(jnp.float32)).astype(jnp.bfloat16)
    ids = jnp.broadcast_to(receiver_row[0].astype(jnp.int16), (LANES, block_rows))
    node = lax.broadcasted_iota(jnp.int16, (LANES, block_rows), 0)
    parts = split(message.astype(jnp.float32) * MESSAGE_SCALE)
    one = jnp.ones((), jnp.bfloat16)
    zero = jnp.zeros((), jnp.bfloat16)
    spread = jnp.concatenate(
        [
            jnp.where(ids == node + jnp.int16(start), one, zero).astype(EIGHT)
            for start in range(0, extended_total, LANES)
        ],
        axis=0,
    )
    sums[...] += joined(product(spread, parts))

    @pl.when(step == pl.num_programs(0) - 1)
    def _():
        owned[...] = sums[:node_total] * (1.0 / MESSAGE_SCALE)
        returned[...] = (sums[node_total:] * (1.0 / MESSAGE_SCALE)).astype(jnp.bfloat16)


def edge_step(count, sender, receiver, receiver_row, latent, nodes, halo, w_in, w_out):
    edge_rows, feature_width = latent.shape
    block_rows = receiver_row.shape[2]
    node_total = nodes.shape[0]
    halo_total = halo.shape[0]
    extended_total = node_total + halo_total
    whole = lambda array: pl.BlockSpec(array.shape, lambda i: (0, 0))
    per_block = lambda width: pl.BlockSpec((block_rows, width), lambda i: (i, 0))
    return pl.pallas_call(
        edge_kernel,
        grid=(edge_rows // block_rows,),
        in_specs=[
            pl.BlockSpec(memory_space=pltpu.SMEM),
            per_block(LANES),
            per_block(LANES),
            pl.BlockSpec((1, 1, block_rows), lambda i: (i, 0, 0)),
            per_block(feature_width),
            whole(nodes),
            whole(halo),
            whole(w_in),
            whole(w_out),
        ],
        out_specs=[
            per_block(feature_width),
            pl.BlockSpec((node_total, feature_width), lambda i: (0, 0)),
            pl.BlockSpec((halo_total, feature_width), lambda i: (0, 0)),
        ],
        out_shape=[
            jax.ShapeDtypeStruct(latent.shape, jnp.bfloat16),
            jax.ShapeDtypeStruct((node_total, feature_width), jnp.float32),
            jax.ShapeDtypeStruct((halo_total, feature_width), jnp.bfloat16),
        ],
        scratch_shapes=[
            pltpu.VMEM((2 * extended_total, feature_width), jnp.float32),
            pltpu.VMEM((2 * extended_total, 2 * feature_width), EIGHT),
            pltpu.SMEM((1,), jnp.float32),
            pltpu.VMEM((extended_total, feature_width), jnp.float32),
        ],
        name="edge_step",
    )(count, sender, receiver, receiver_row, latent, nodes, halo, w_in, w_out)


def across(block, step_of_core):
    domains = lax.axis_size("dom")
    cores = lax.axis_size("tp")
    pairs = [
        (p * cores + t, ((p + step_of_core[t]) % domains) * cores + t)
        for p in range(domains)
        for t in range(cores)
    ]
    return lax.ppermute(block, ("dom", "tp"), pairs)


def swap(array):
    return from_behind(array, "tp", 1)


def in_core_order(mine, other, axis):
    first = lax.axis_index("tp") == 0
    return jnp.concatenate(
        [jnp.where(first, mine, other), jnp.where(first, other, mine)], axis=axis
    )


def local(
    node_latent,
    edge_latent,
    edge_sender,
    edge_receiver,
    edge_count,
    send_index,
    edge_in,
    edge_out,
    node_in,
    node_out,
):
    feature_width = node_latent.shape[1]
    node_total = node_latent.shape[0]
    edge_rows = edge_latent.shape[0]
    block_rows = min(1024, edge_rows)
    peers, slot = send_index.shape[1:]
    flat_index = send_index[0].reshape(-1)
    node_ids = jnp.arange(node_total, dtype=jnp.int32)
    cores = lax.axis_size("tp")
    per_core = peers // cores
    own_rows = per_core * slot
    own_steps = [
        tuple(neighbour_offsets[t * per_core + j] for t in range(cores)) for j in range(per_core)
    ]
    core = lax.axis_index("tp")
    own_index = lax.dynamic_slice_in_dim(flat_index, core * own_rows, own_rows)
    pick_table = (own_index[:, None] == node_ids[None, :]).astype(jnp.bfloat16)
    spread_table = (node_ids[:, None] == own_index[None, :]).astype(jnp.bfloat16)

    def placed(ids):
        slot_at = (ids - node_total + (cores - core) * own_rows) % (peers * slot)
        return jnp.where(ids < node_total, ids, node_total + slot_at)

    edge_sender = placed(edge_sender)
    edge_receiver = placed(edge_receiver)
    wide = lambda ids: jnp.broadcast_to(ids.astype(jnp.int16)[:, None], (edge_rows, LANES))
    sender = wide(edge_sender)
    receiver = wide(edge_receiver)
    receiver_row = edge_receiver.reshape(edge_rows // block_rows, 1, block_rows)
    full_in = jnp.concatenate([edge_in, swap(edge_in)], axis=2)
    full_out = jnp.concatenate([edge_out, swap(edge_out)], axis=1)
    node_first = in_core_order(node_in, swap(node_in), 2)
    node_second = in_core_order(node_out, swap(node_out), 1)
    nodes_now = node_latent
    edges_now = edge_latent
    for layer in range(LAYERS):
        picked = product(pick_table, nodes_now).astype(jnp.bfloat16)
        fetched = [
            across(picked[j * slot : (j + 1) * slot], own_steps[j]) for j in range(per_core)
        ]
        fetched = jnp.concatenate(fetched, axis=0)
        halo = jnp.concatenate([fetched, swap(fetched)], axis=0)
        edges_now, owned, returned = edge_step(
            edge_count, sender, receiver, receiver_row, edges_now, nodes_now, halo,
            full_in[layer], full_out[layer],
        )
        sums = returned[:own_rows].astype(jnp.float32) + swap(returned[own_rows:]).astype(
            jnp.float32
        )
        sums = sums.astype(jnp.bfloat16)
        arrived = [
            across(sums[j * slot : (j + 1) * slot], [-o for o in own_steps[j]])
            for j in range(per_core)
        ]
        mine = owned + product(spread_table, jnp.concatenate(arrived, axis=0))
        mine = mine.astype(jnp.bfloat16)
        other = swap(mine)
        aggregate = (mine.astype(jnp.float32) + other.astype(jnp.float32)).astype(jnp.bfloat16)
        linear = product(nodes_now, node_first[layer][:feature_width]) + product(
            aggregate, node_first[layer][feature_width:]
        )
        hidden = jnp.maximum(linear, 0.0).astype(jnp.bfloat16)
        update = layer_norm(product(hidden, node_second[layer]))
        nodes_now = (nodes_now.astype(jnp.float32) + update).astype(jnp.bfloat16)
    return (nodes_now, edges_now)


def solution(mesh):
    return jax.shard_map(
        local,
        mesh=mesh,
        in_specs=(
            P("dom", None),
            P(("dom", "tp"), None),
            P(("dom", "tp")),
            P(("dom", "tp")),
            P(("dom", "tp")),
            P("dom", None, None),
            P(None, None, "tp"),
            P(None, "tp", None),
            P(None, None, "tp"),
            P(None, "tp", None),
        ),
        out_specs=(P("dom", None), P(("dom", "tp"), None)),
        check_vma=False,
    )
```
